32 devices in a mesh: dp: 8 (over y, x, core), tensor: 4 (over z).
Axes of the slice: x: 2, y: 2, z: 4, core: 2. Of those that a mesh axis runs over, the one named last changes fastest.
Arguments:
- memory: bfloat16 [12288, 1280], P('dp'), may hold values from -6 to 6
- hidden: bfloat16 [12288, 2560], P('dp', 'tensor'), may hold values from -6 to 6
- grad_out: bfloat16 [12288, 2560], P('dp', 'tensor'), may hold values from -6 to 6
- key_weight: bfloat16 [1280, 2560], P('dp', 'tensor'), may hold values from -0.15625 to 0.15625
- value_weight: bfloat16 [1280, 2560], P('dp', 'tensor'), may hold values from -0.15625 to 0.15625
- row_ids: int32 [12288, 5], P('dp'), may hold values from 0 to 65535, as said below
- embed_table: float32 [65536, 256], P(('dp', 'tensor')), may hold values from -6 to 6
- first_moment: float32 [65536, 256], P(('dp', 'tensor')), may hold values from -0.6 to 0.6
- second_moment: float32 [65536, 256], P(('dp', 'tensor')), may hold values from 0.001 to 0.1
Outputs:
- key_weight_grad: float32 [1280, 2560], P('dp', 'tensor')
- value_weight_grad: float32 [1280, 2560], P('dp', 'tensor')
- new_table: float32 [65536, 256], P(('dp', 'tensor'))
- new_first: float32 [65536, 256], P(('dp', 'tensor'))
- new_second: float32 [65536, 256], P(('dp', 'tensor'))
The draws below stay inside these ranges and needn't reach their ends.
Inputs may be any that keep to these rules, and one draw needn't show every extreme that they name: `row_ids`: the table's rows fall into 32 owners of 2048 consecutive rows each. Taking the tokens in aligned blocks of 384 consecutive tokens with all their 5 ids, at most 180 ids of one block fall in one owner's rows, and in every block some owner gets exactly 180 of them.
All inputs are finite; a program needn't handle non-finite values.
Results may differ from the reference program's by a relative error of at most 0.0043.
Values may be sent and summed in bfloat16 or wider, within the bound.
A program may use at most 128 MiB of HBM per device.

```python
import math
import jax
import jax.numpy as jnp
from jax import lax

D = 2560
ROW_W = 256
LOOKUPS = 5
MEM = 1280
ROWS_DEV = 2048
BLOCK = 384
CAP = 180
TOKENS = 12288
ROWS = 65536
DEVICES = 32


def block_ids(block_key):
    entries = BLOCK * LOOKUPS
    owners = DEVICES
    slots = owners * CAP
    keys = jax.random.split(block_key, 5)
    loads = jax.random.randint(keys[0], (owners,), 1, CAP + 1)
    hottest = jax.random.randint(keys[1], (), 0, owners)
    slot_index = jnp.arange(slots, dtype=jnp.int32)
    slot_owner = slot_index // CAP
    slot_copy = slot_index % CAP
    tier = jnp.where(slot_owner == hottest, 2, jnp.where(slot_copy < loads[slot_owner], 1, 0))
    noise = jax.random.randint(keys[2], (slots,), 0, 2048)
    score = tier * 16777216 + noise * 8192 + slot_index
    chosen = lax.top_k(score, entries)[1]
    owner_of = jax.random.permutation(keys[3], chosen // CAP)
    local_row = jax.random.randint(keys[4], (entries,), 0, ROWS_DEV)
    return (owner_of * ROWS_DEV + local_row).astype(jnp.int32)


def draw_row_ids(key, part):
    count = TOKENS // BLOCK
    keys = jax.random.split(jax.random.fold_in(key, 7), count)
    table_ids = jax.vmap(block_ids)(keys)
    return table_ids.reshape(TOKENS, LOOKUPS).astype(jnp.int32)


def block_levels(own_key, extent, cuts, low, top_value):
    factor_of = 1.0
    for position, blocks in cuts:
        steps = jax.random.uniform(jax.random.fold_in(jax.random.fold_in(own_key, 6), position), (blocks,), jnp.float32, low / len(cuts), top_value / len(cuts))
        factor_of = factor_of * jnp.repeat(jnp.exp(steps), extent[position] // blocks).reshape((-1,) + (1,) * (len(extent) - 1 - position))
    return factor_of


def normal_values(rng, dims, spread, reach, shards=(), kind=jnp.bfloat16):
    values = spread * jax.random.normal(rng, dims, jnp.float32)
    if shards:
        values = values * block_levels(rng, dims, shards, -0.22, 0.18)
    return jnp.clip(values, -reach, reach).astype(kind)


def setup_inputs(seed: int = 0) -> dict:
    streams_of = jax.random.split(jax.random.key(seed), 10)
    return {
        "memory": normal_values(streams_of[0], (TOKENS, MEM), 1.0, 6.0, ((0, 8),)),
        "hidden": normal_values(streams_of[1], (TOKENS, D), 1.0, 6.0, ((0, 8), (1, 4))),
        "grad_out": normal_values(streams_of[2], (TOKENS, D), 1.0, 6.0, ((0, 8), (1, 4))),
        "key_weight": normal_values(streams_of[3], (MEM, D), MEM ** -0.5, 0.15625, ((0, 8), (1, 4))),
        "value_weight": normal_values(streams_of[4], (MEM, D), MEM ** -0.5, 0.15625, ((0, 8), (1, 4))),
        "row_ids": draw_row_ids(jax.random.fold_in(streams_of[9], 71), 0),
        "embed_table": normal_values(streams_of[6], (ROWS, ROW_W), 1.0, 6.0, ((0, 32),), jnp.float32),
        "first_moment": normal_values(streams_of[7], (ROWS, ROW_W), 0.1, 0.6, ((0, 32),), jnp.float32),
        "second_moment": jnp.clip(jnp.exp(math.log(0.1) - 4.6051702 * jax.random.uniform(streams_of[8], (ROWS, ROW_W), jnp.float32) ** block_levels(streams_of[8], (ROWS, ROW_W), ((0, 32),), -0.2, 0.2)), 0.001, 0.1),
    }


beta_one = 0.9
beta_two = 0.999
learn_rate = 0.01
adam_eps = 1e-08
norm_eps = 1e-06
correct_one = 0.9999734386011124
correct_two = 0.0952078528863

def adam_update(table_grad, embed_table, first_moment, second_moment):
    new_first = beta_one * first_moment + (1.0 - beta_one) * table_grad
    new_second = beta_two * second_moment + (1.0 - beta_two) * table_grad * table_grad
    stepped = new_first / correct_one / (jnp.sqrt(new_second / correct_two) + adam_eps)
    return (embed_table - learn_rate * stepped, new_first, new_second)

def reference(memory, hidden, grad_out, key_weight, value_weight, row_ids, embed_table, first_moment, second_moment):
    key_proj = jnp.dot(memory, key_weight, preferred_element_type=jnp.float32)
    value_proj = jnp.dot(memory, value_weight, preferred_element_type=jnp.float32)
    hidden_float = hidden.astype(jnp.float32)
    grad_float = grad_out.astype(jnp.float32)
    root_width = math.sqrt(D)
    key_scale = jnp.sqrt(lax.optimization_barrier(jnp.mean(key_proj * key_proj, axis=1, keepdims=True)) + norm_eps)
    gate_score = lax.optimization_barrier(jnp.sum(hidden_float * key_proj, axis=1, keepdims=True)) / (key_scale * root_width)
    gate_value = jax.nn.sigmoid(gate_score)
    gate_grad = gate_value * (1.0 - gate_value) * lax.optimization_barrier(jnp.sum(grad_float * value_proj, axis=1, keepdims=True))
    value_grad = (gate_value * grad_float).astype(jnp.bfloat16)
    key_grad = (gate_grad * (hidden_float / (key_scale * root_width) - gate_score * key_proj / (D * key_scale * key_scale))).astype(jnp.bfloat16)
    contract = (((0,), (0,)), ((), ()))
    key_weight_grad = lax.dot_general(memory, key_grad, contract, preferred_element_type=jnp.float32)
    value_weight_grad = lax.dot_general(memory, value_grad, contract, preferred_element_type=jnp.float32)
    memory_grad = jnp.dot(key_grad, key_weight.T, preferred_element_type=jnp.float32) + jnp.dot(value_grad, value_weight.T, preferred_element_type=jnp.float32)
    memory_grad = memory_grad.astype(jnp.bfloat16)
    pieces = memory_grad.reshape(-1, ROW_W).astype(jnp.float32)
    table_grad = jnp.zeros(embed_table.shape, jnp.float32).at[row_ids.reshape(-1).astype(jnp.int32)].add(pieces)
    new_table, new_first, new_second = adam_update(table_grad, embed_table, first_moment, second_moment)
    return (key_weight_grad, value_weight_grad, new_table, new_first, new_second)
```

```python
import math

import jax
import jax.numpy as jnp
from jax import lax
from jax.experimental import pallas as pl
from jax.experimental.pallas import tpu as pltpu
from jax.sharding import PartitionSpec as P

beta_one = 0.9
beta_two = 0.999
learn_rate = 0.01
adam_eps = 1e-08
norm_eps = 1e-06
correct_one = 0.9999734386011124
correct_two = 0.0952078528863


def adam_update(table_grad, embed_table, first_moment, second_moment):
    new_first = beta_one * first_moment + (1.0 - beta_one) * table_grad
    new_second = beta_two * second_moment + (1.0 - beta_two) * table_grad * table_grad
    stepped = new_first / correct_one / (jnp.sqrt(new_second / correct_two) + adam_eps)
    return (embed_table - learn_rate * stepped, new_first, new_second)


f32 = jnp.float32
bf16 = jnp.bfloat16
lanes = 128
sublanes = 8


def full_spec(shape):
    return pl.BlockSpec(shape, lambda i: (0,) * len(shape))


def project_kernel(memory_ref, weights_ref, hidden_ref, grad_ref, key_ref, sums_ref):
    width = hidden_ref.shape[1]
    tile = memory_ref.shape[0]
    proj = jnp.dot(memory_ref[...], weights_ref[...], preferred_element_type=f32)
    key_proj = proj[:, :width]
    key_ref[...] = key_proj
    square = jnp.sum(key_proj * key_proj, axis=1, keepdims=True)
    cross = jnp.sum(hidden_ref[...].astype(f32) * key_proj, axis=1, keepdims=True)
    output = jnp.sum(grad_ref[...].astype(f32) * proj[:, width:], axis=1, keepdims=True)
    lane = lax.broadcasted_iota(jnp.int32, (tile, lanes), 1)
    packed = jnp.where(
        lane == 0, square, jnp.where(lane == 1, cross, jnp.where(lane == 2, output, 0.0))
    )
    sums_ref[...] = packed.T[:sublanes, :]


def grads_kernel(
    model_width, sums_ref, hidden_ref, grad_ref, key_ref, weights_ref, both_ref, piece_ref
):
    width = hidden_ref.shape[1]
    tile = hidden_ref.shape[0]
    sums = sums_ref[0]
    for part in range(1, sums_ref.shape[0]):
        sums = sums + sums_ref[part]
    root_width = math.sqrt(model_width)
    key_scale = jnp.sqrt(sums[0:1] / model_width + norm_eps)
    gate_score = sums[1:2] / (key_scale * root_width)
    gate_value = 1.0 / (1.0 + jnp.exp(-gate_score))
    gate_grad = gate_value * (1.0 - gate_value) * sums[2:3]
    hidden_factor = gate_grad / (key_scale * root_width)
    key_factor = gate_grad * (gate_score / (model_width * key_scale * key_scale))
    row = lax.broadcasted_iota(jnp.int32, (lanes, tile), 0)
    factors = jnp.where(
        row == 0, hidden_factor, jnp.where(row == 1, key_factor, gate_value)
    ).T
    key_grad = (
        factors[:, 0:1] * hidden_ref[...].astype(f32) - factors[:, 1:2] * key_ref[...]
    ).astype(bf16)
    value_grad = (factors[:, 2:3] * grad_ref[...].astype(f32)).astype(bf16)
    both_ref[:, :width] = key_grad
    both_ref[:, width:] = value_grad
    contract = (((1,), (1,)), ((), ()))
    piece_ref[...] = lax.dot_general(
        both_ref[...], weights_ref[...], contract, preferred_element_type=f32
    ).astype(bf16)


def dispatch_kernel(lookups, row_width, slot_ref, total_ref, out_ref):
    block = total_ref.shape[0]
    tile = out_ref.shape[0]
    slot = lax.broadcasted_iota(jnp.int32, (tile, block), 0) + pl.program_id(0) * tile
    rows = jnp.zeros((tile, row_width), f32)
    for lookup in range(lookups):
        hot = jnp.where(slot == slot_ref[:, lookup * block : (lookup + 1) * block], 1.0, 0.0)
        rows = rows + jnp.dot(
            hot.astype(bf16),
            total_ref[:, lookup * row_width : (lookup + 1) * row_width],
            preferred_element_type=f32,
        )
    out_ref[...] = rows.astype(bf16)


def combine_kernel(
    chunk, ids_ref, rows_ref, table_ref, first_ref, second_ref, new_table, new_first, new_second
):
    tile, row_width = table_ref.shape
    row = lax.broadcasted_iota(jnp.int32, (tile, chunk), 0) + pl.program_id(0) * tile
    table_grad = jnp.zeros((tile, row_width), f32)
    for start in range(0, rows_ref.shape[0], chunk):
        hot = jnp.where(row == ids_ref[:, start : start + chunk], 1.0, 0.0)
        table_grad = table_grad + jnp.dot(
            hot.astype(bf16), rows_ref[start : start + chunk, :], preferred_element_type=f32
        )
    new_table[...], new_first[...], new_second[...] = adam_update(
        table_grad, table_ref[...], first_ref[...], second_ref[...]
    )


def divisor(count, choices):
    return next((c for c in choices if count % c == 0), count)


def body(
    memory,
    hidden,
    grad_out,
    key_weight,
    value_weight,
    row_ids,
    embed_table,
    first_moment,
    second_moment,
):
    dp_count = lax.axis_size("dp")
    tensor_count = lax.axis_size("tensor")
    tokens, mem = memory.shape
    width = hidden.shape[1]
    model_width = width * tensor_count
    rows_dev, row_width = embed_table.shape
    lookups = row_ids.shape[1]
    block = tokens // tensor_count
    entries = block * lookups
    owners = dp_count * tensor_count
    capacity = max(2, 3 * entries // owners)
    slots = owners * capacity

    weights = lax.all_gather(
        jnp.concatenate([key_weight, value_weight], axis=1), "dp", axis=0, tiled=True
    )

    my_ids = lax.dynamic_slice_in_dim(row_ids, lax.axis_index("tensor") * block, block, 0)
    my_ids = my_ids.T.reshape(-1)
    owner_of = my_ids // rows_dev
    local_row = my_ids % rows_dev
    owner_hits = (owner_of[:, None] == jnp.arange(owners, dtype=jnp.int32)[None, :]).astype(bf16)
    earlier = (jnp.arange(entries)[None, :] < jnp.arange(entries)[:, None]).astype(bf16)
    before_counts = jnp.dot(earlier, owner_hits, preferred_element_type=f32)
    slot_rank = jnp.sum(before_counts * owner_hits.astype(f32), axis=1).astype(jnp.int32)
    slot_index = owner_of * capacity + slot_rank
    rank_hits = slot_rank[:, None] == jnp.arange(capacity, dtype=jnp.int32)[None, :]
    code = local_row + 1
    coded = jnp.concatenate(
        [
            jnp.where(rank_hits, (code // 64)[:, None], 0),
            jnp.where(rank_hits, (code % 64)[:, None], 0),
        ],
        axis=1,
    ).astype(bf16)
    sent_codes = lax.dot_general(
        owner_hits, coded, (((0,), (0,)), ((), ())), preferred_element_type=f32
    ).astype(jnp.int32)
    send_ids = sent_codes[:, :capacity] * 64 + sent_codes[:, capacity:] - 1
    got_ids = lax.all_to_all(
        send_ids, ("dp", "tensor"), split_axis=0, concat_axis=0, tiled=True
    ).reshape(1, slots)

    tile = divisor(tokens, (256, 128))
    steps = tokens // tile
    token_spec = lambda columns: pl.BlockSpec((tile, columns), lambda i: (i, 0))
    key_proj, sums = pl.pallas_call(
        project_kernel,
        grid=(steps,),
        in_specs=[token_spec(mem), full_spec((mem, 2 * width)), token_spec(width), token_spec(width)],
        out_specs=[token_spec(width), pl.BlockSpec((sublanes, tile), lambda i: (0, i))],
        out_shape=[
            jax.ShapeDtypeStruct((tokens, width), f32),
            jax.ShapeDtypeStruct((sublanes, tokens), f32),
        ],
        cost_estimate=pl.CostEstimate(
            flops=4 * tokens * mem * width, bytes_accessed=12 * tokens * width, transcendentals=0
        ),
        name="project",
    )(memory, weights, hidden, grad_out)
    all_sums = lax.all_gather(sums, "tensor", axis=0)
    both_grads, pieces = pl.pallas_call(
        lambda *refs: grads_kernel(model_width, *refs),
        grid=(steps,),
        in_specs=[
            pl.BlockSpec((tensor_count, sublanes, tile), lambda i: (0, 0, i)),
            token_spec(width),
            token_spec(width),
            token_spec(width),
            full_spec((mem, 2 * width)),
        ],
        out_specs=[token_spec(2 * width), token_spec(mem)],
        out_shape=[
            jax.ShapeDtypeStruct((tokens, 2 * width), bf16),
            jax.ShapeDtypeStruct((tokens, mem), bf16),
        ],
        cost_estimate=pl.CostEstimate(
            flops=4 * tokens * mem * width, bytes_accessed=16 * tokens * width, transcendentals=0
        ),
        name="grads",
    )(all_sums, hidden, grad_out, key_proj, weights)
    total = lax.psum_scatter(pieces, "tensor", scatter_dimension=0, tiled=True)
    weight_grads = lax.psum_scatter(
        lax.dot_general(
            memory, both_grads, (((0,), (0,)), ((), ())), preferred_element_type=f32
        ).astype(bf16),
        "dp",
        scatter_dimension=0,
        tiled=True,
    ).astype(f32)

    slot_tile = divisor(slots, (720, 960, 640, 128))
    send_rows = pl.pallas_call(
        lambda *refs: dispatch_kernel(lookups, row_width, *refs),
        grid=(slots // slot_tile,),
        in_specs=[full_spec((1, entries)), full_spec((block, mem))],
        out_specs=pl.BlockSpec((slot_tile, row_width), lambda i: (i, 0)),
        out_shape=jax.ShapeDtypeStruct((slots, row_width), bf16),
        cost_estimate=pl.CostEstimate(
            flops=2 * slots * entries * row_width, bytes_accessed=4 * slots * row_width,
            transcendentals=0,
        ),
        name="dispatch",
    )(slot_index.reshape(1, entries), total)
    got_rows = lax.all_to_all(
        send_rows.reshape(owners, capacity, row_width),
        ("dp", "tensor"),
        split_axis=0,
        concat_axis=0,
        tiled=True,
    ).reshape(slots, row_width)
    row_tile = divisor(rows_dev, (256, 128))
    row_spec = pl.BlockSpec((row_tile, row_width), lambda i: (i, 0))
    table_shape = jax.ShapeDtypeStruct((rows_dev, row_width), f32)
    chunk = divisor(slots, (1152, 960, 640, 128))
    new_table, new_first, new_second = pl.pallas_call(
        lambda *refs: combine_kernel(chunk, *refs),
        grid=(rows_dev // row_tile,),
        in_specs=[full_spec((1, slots)), full_spec((slots, row_width)), row_spec, row_spec, row_spec],
        out_specs=[row_spec] * 3,
        out_shape=[table_shape] * 3,
        cost_estimate=pl.CostEstimate(
            flops=2 * slots * rows_dev * row_width, bytes_accessed=24 * rows_dev * row_width,
            transcendentals=0,
        ),
        name="combine",
    )(got_ids, got_rows, embed_table, first_moment, second_moment)
    return (weight_grads[:, :width], weight_grads[:, width:], new_table, new_first, new_second)


def solution(mesh):
    return jax.shard_map(
        body,
        mesh=mesh,
        in_specs=(
            P("dp", None),
            P("dp", "tensor"),
            P("dp", "tensor"),
            P("dp", "tensor"),
            P("dp", "tensor"),
            P("dp", None),
            P(("dp", "tensor"), None),
            P(("dp", "tensor"), None),
            P(("dp", "tensor"), None),
        ),
        out_specs=(
            P("dp", "tensor"),
            P("dp", "tensor"),
            P(("dp", "tensor"), None),
            P(("dp", "tensor"), None),
            P(("dp", "tensor"), None),
        ),
        check_vma=False,
    )
```
